256 devices in a mesh: groups: 2 (over z), seq: 16 (over y, core), head: 8 (over x).
Axes of the slice: x: 8, y: 8, z: 2, core: 2. Of those that a mesh axis runs over, the one named last changes fastest.
The devices are a block of a 8x8x16 slice.
Arguments:
- queries: bfloat16 [65536, 3072], P(('groups', 'seq'), 'head'), parts along dimension 0, may hold values from -30 to 30
- keys_values: bfloat16 [2, 65536, 3072], P(None, ('groups', 'seq'), 'head'), parts along dimension 1, may hold values from -10 to 10
- shot_bounds: int32 [256, 2], P(('groups', 'seq')), parts along dimension 0, may hold values from 0 to 128, as said below
- routes: int32 [256, 2], P(('groups', 'seq')), parts along dimension 0, may hold values from 0 to 127, as said below
Outputs:
- attended: bfloat16 [65536, 3072], P(('groups', 'seq'), 'head'), parts along dimension 0
The draws below stay inside these ranges and needn't reach their ends.
There are 2 independent parts, one for each index of `groups`. The reference program is written for one: setup_inputs(seed, part) draws one part's arguments, and reference() takes and returns one part's arrays. A program takes and returns all parts, laid end to end along the dimension named above; each array names one. Nothing has to cross between parts.
Inputs may be any that keep to these rules, and one draw needn't show every extreme that they name: Each shot is a run of 1 to 3 stretches; shots tile the stretches in order; for stretch c, shot_bounds[c] = (s, e) with s <= c < e is the run that holds c; in every draw some shot has 3 stretches. `routes`: stretch d * 8 + i is held by device d of seq. Of the 16 entries of the rows of one device, at most 2 name stretches held by any one device, and in every draw every device has some such device named exactly 2 times.
All inputs are finite; a program needn't handle non-finite values.
Results may differ from the reference program's by a relative error of at most 0.0033.
Values may be sent and summed in bfloat16 or wider, within the bound.
A program may use at most 128 MiB of HBM per device.

```python
import jax
import jax.numpy as jnp
from jax import lax

STRETCH = 256
HEADS = 24
HEAD_SIZE = 128
SHOT_MAX = 3
TOPK = 2
STRETCHES_DEV = 8
NCH = 128
TOKENS = 32768
HD = 3072
CAP = 2


def draw_queries(key, part):
    drawn = 2.5 * jax.random.normal(jax.random.fold_in(key, 11), (TOKENS, HD), jnp.float32)
    return jnp.clip(drawn, -30.0, 30.0).astype(jnp.bfloat16)


def draw_keys_values(key, part):
    row_part = jax.random.normal(jax.random.fold_in(key, 21), (2, TOKENS, HD), jnp.float32)
    stretch_part = jax.random.normal(jax.random.fold_in(key, 22), (2, NCH, 1, HD), jnp.float32)
    mixture = 0.6 * row_part + 0.8 * jnp.broadcast_to(stretch_part, (2, NCH, STRETCH, HD)).reshape(2, TOKENS, HD)
    return jnp.clip(mixture, -10.0, 10.0).astype(jnp.bfloat16)


def draw_shot_bounds(key, part):
    lengths = jax.random.randint(jax.random.fold_in(key, 1), (NCH,), 1, SHOT_MAX + 1)
    longest = jax.random.randint(jax.random.fold_in(key, 2), (), 0, max(1, NCH // (2 * SHOT_MAX)))
    lengths = jnp.where(jnp.arange(NCH) == longest, SHOT_MAX, lengths).astype(jnp.int32)
    shot_ends = jnp.cumsum(lengths).astype(jnp.int32)
    shot_starts = shot_ends - lengths
    position = jnp.arange(NCH, dtype=jnp.int32)
    shot_number = jnp.sum((shot_ends[None, :] <= position[:, None]).astype(jnp.int32), axis=1)
    one_hot = (position[None, :] == shot_number[:, None]).astype(jnp.int32)
    start = jnp.sum(one_hot * shot_starts[None, :], axis=1)
    finish = jnp.minimum(jnp.sum(one_hot * shot_ends[None, :], axis=1), NCH)
    return jnp.stack([start, finish], axis=1).astype(jnp.int32)


def draw_routes(key, part):
    device_total = NCH // STRETCHES_DEV
    request_total = STRETCHES_DEV * TOPK
    slot_total = device_total * CAP

    def device_routes(device):
        device_key = jax.random.fold_in(key, 100 + device)
        full_owner = jax.random.randint(jax.random.fold_in(device_key, 1), (), 0, device_total)
        shuffled = jax.random.permutation(jax.random.fold_in(device_key, 2), slot_total).astype(jnp.int32)
        slot_owner = jnp.arange(slot_total, dtype=jnp.int32) // CAP
        priority = jnp.where(slot_owner == full_owner, shuffled - slot_total, shuffled)
        ranked = jnp.argsort(priority, stable=True)[:request_total]
        owners = slot_owner[ranked]
        owners = owners[jax.random.permutation(jax.random.fold_in(device_key, 3), request_total)]
        locals_drawn = jax.random.randint(jax.random.fold_in(device_key, 4), (request_total,), 0, STRETCHES_DEV)
        return (owners * STRETCHES_DEV + locals_drawn).reshape(STRETCHES_DEV, TOPK)
    every = jax.vmap(device_routes)(jnp.arange(device_total))
    return every.reshape(NCH, TOPK).astype(jnp.int32)


def setup_inputs(seed: int = 0, part: int = 0) -> dict:
    key_list = jax.random.split(jax.random.key(seed), 5)
    own_keys = jax.random.split(jax.random.fold_in(key_list[4], part), 5)
    queries = draw_queries(jax.random.fold_in(jax.random.fold_in(key_list[4], part), 71), part)
    keys_values = draw_keys_values(jax.random.fold_in(jax.random.fold_in(key_list[4], part), 71), part)
    shot_bounds = draw_shot_bounds(jax.random.fold_in(jax.random.fold_in(key_list[4], part), 71), part)
    routes = draw_routes(jax.random.fold_in(jax.random.fold_in(key_list[4], part), 71), part)
    return {"queries": queries, "keys_values": keys_values, "shot_bounds": shot_bounds, "routes": routes}


NEG_FILL = -1.0e30


def spread_heads(scales):
    return jnp.repeat(jnp.swapaxes(scales, -1, -2), HEAD_SIZE, axis=-1)


def partial_block(query_rows, key_rows, value_rows):
    batch_count, query_count = query_rows.shape[0], query_rows.shape[1]
    key_count = key_rows.shape[1]
    query_heads = query_rows.astype(jnp.float32).reshape(batch_count, query_count, HEADS, HEAD_SIZE)
    key_heads = key_rows.astype(jnp.float32).reshape(batch_count, key_count, HEADS, HEAD_SIZE)
    value_heads = value_rows.astype(jnp.float32).reshape(batch_count, key_count, HEADS, HEAD_SIZE)
    scores = jnp.einsum("bqhd,bkhd->bhqk", query_heads, key_heads, precision=lax.Precision.HIGHEST) * (HEAD_SIZE ** -0.5)
    peaks = jnp.max(scores, axis=-1)
    weights = jnp.exp(scores - peaks[..., None]).astype(jnp.bfloat16)
    weights = lax.optimization_barrier(weights).astype(jnp.float32)
    totals = jnp.sum(weights, axis=-1)
    blended = jnp.einsum("bhqk,bkhd->bqhd", weights, value_heads, precision=lax.Precision.HIGHEST)
    return peaks, totals, blended.reshape(batch_count, query_count, HEADS * HEAD_SIZE)


def reference(queries, keys_values, shot_bounds, routes):
    rim_stretches = SHOT_MAX - 1
    kv_stretches = keys_values.reshape(2, NCH, STRETCH, HD)
    pooled = jnp.mean(kv_stretches, axis=2, dtype=jnp.float32).astype(jnp.bfloat16)
    padded = jnp.pad(keys_values, ((0, 0), (rim_stretches * STRETCH, rim_stretches * STRETCH), (0, 0)))
    query_stretches = queries.reshape(NCH, STRETCH, HD)
    block_count = SHOT_MAX + TOPK

    def stretch_output(inputs):
        query_stretch, bounds, picks = inputs
        offset = ((bounds[0] + rim_stretches) * STRETCH).astype(jnp.int32)
        window = lax.dynamic_slice_in_dim(padded, offset, SHOT_MAX * STRETCH, 1).reshape(2, SHOT_MAX, STRETCH, HD)
        routed = kv_stretches[:, picks.astype(jnp.int32)]
        key_blocks = jnp.concatenate([window[0], routed[0]], axis=0)
        value_blocks = jnp.concatenate([window[1], routed[1]], axis=0)
        peaks, totals, blended = partial_block(jnp.broadcast_to(query_stretch[None], (block_count, STRETCH, HD)), key_blocks, value_blocks)
        usable = jnp.concatenate([jnp.arange(SHOT_MAX) < bounds[1] - bounds[0], jnp.ones((TOPK,), bool)])
        peaks = jnp.where(usable[:, None, None], peaks, NEG_FILL)
        pool_peaks, pool_totals, pool_blended = partial_block(query_stretch[None], pooled[0][None], pooled[1][None])
        peaks = jnp.concatenate([peaks, pool_peaks], axis=0)
        totals = jnp.concatenate([totals, pool_totals], axis=0)
        blended = jnp.concatenate([blended, pool_blended], axis=0)
        highest = jnp.max(peaks, axis=0)
        factors = jnp.exp(peaks - highest[None])
        denominator = jnp.sum(factors * totals, axis=0)
        numerator = jnp.sum(spread_heads(factors) * blended, axis=0)
        return (numerator / spread_heads(denominator)).astype(jnp.bfloat16)

    result = lax.map(stretch_output, (query_stretches, shot_bounds, routes))
    return result.reshape(TOKENS, HD)
```

```python
import functools

import jax
import jax.numpy as jnp
from jax import lax
from jax.experimental import pallas as pl
from jax.experimental.pallas import tpu as pltpu
from jax.sharding import PartitionSpec as P

STRETCH = 256
HEAD_SIZE = 128
SHOT_MAX = 3
TOPK = 2
RIM = SHOT_MAX - 1
BLOCKS = SHOT_MAX + TOPK
NEG_FILL = -1e30
LOG2_E = 1.4426950408889634
ANY = pl.BlockSpec(memory_space=pl.ANY)


def edge_stretches(keys_values, width):
    size, length = lax.axis_size("seq"), keys_values.shape[1]
    up = [(i, (i + 1) % size) for i in range(size)]
    down = [(j, i) for i, j in up]
    before = lax.ppermute(keys_values[:, length - width :], "seq", up)
    after = lax.ppermute(keys_values[:, :width], "seq", down)
    return before, after


def attend_kernel(
    tab_ref, q_ref, pool_ref, own_ref, before_ref, after_ref, routed_ref, out_ref, blocks, sems
):
    step, steps = pl.program_id(0), pl.num_programs(0)

    def each_source(i, b, slot, act):
        source, index = tab_ref[i, 2 * b], tab_ref[i, 2 * b + 1]
        target, sem = blocks.at[slot, b], sems.at[slot, b]

        def rows(ref):
            return ref.at[:, pl.ds(pl.multiple_of(index * STRETCH, STRETCH), STRETCH), :]

        for number, view in enumerate(
            (rows(own_ref), rows(before_ref), rows(after_ref), routed_ref.at[index])
        ):
            @pl.when(source == number)
            def _():
                act(pltpu.make_async_copy(view, target, sem))

    def start(i, slot):
        for b in range(BLOCKS):
            each_source(i, b, slot, lambda copy: copy.start())

    @pl.when(step == 0)
    def _():
        start(0, 0)

    @pl.when(step + 1 < steps)
    def _():
        start(step + 1, lax.rem(step + 1, 2))

    slot = lax.rem(step, 2)
    for b in range(BLOCKS):
        pltpu.make_async_copy(
            own_ref.at[:, pl.ds(0, STRETCH), :], blocks.at[slot, b], sems.at[slot, b]
        ).wait()
    live = tab_ref[step, 2 * BLOCKS]
    heads = q_ref.shape[1] // HEAD_SIZE
    factor = LOG2_E * HEAD_SIZE ** (-0.5)
    for head in range(heads):
        columns = slice(head * HEAD_SIZE, (head + 1) * HEAD_SIZE)
        queries = q_ref[:, columns]

        def scores_of(keys):
            return lax.dot_general(
                queries, keys, (((1,), (1,)), ((), ())), preferred_element_type=jnp.float32
            )

        scores = [scores_of(pool_ref[0, :, columns])]
        for b in range(BLOCKS):
            score = scores_of(blocks[slot, b, 0, :, columns])
            if 0 < b < SHOT_MAX:
                score = jnp.where(b < live, score, NEG_FILL)
            scores.append(score)
        peak = functools.reduce(
            jnp.maximum, [jnp.max(score, axis=1, keepdims=True) for score in scores]
        )
        total, blended = 0.0, 0.0
        for b, score in enumerate(scores):
            weights = jnp.exp2((score - peak) * factor).astype(jnp.bfloat16)
            total += jnp.sum(weights.astype(jnp.float32), axis=1, keepdims=True)
            values = pool_ref[1, :, columns] if b == 0 else blocks[slot, b - 1, 1, :, columns]
            blended += jnp.dot(weights, values, preferred_element_type=jnp.float32)
        out_ref[:, columns] = (blended / total).astype(jnp.bfloat16)


def attend(table, queries, pooled, own, before, after, routed):
    rows, width = queries.shape
    steps = rows // STRETCH
    block = pl.BlockSpec((STRETCH, width), lambda i, tab: (i, 0))
    return pl.pallas_call(
        attend_kernel,
        out_shape=jax.ShapeDtypeStruct((rows, width), jnp.bfloat16),
        grid_spec=pltpu.PrefetchScalarGridSpec(
            num_scalar_prefetch=1,
            grid=(steps,),
            in_specs=[
                block,
                pl.BlockSpec(pooled.shape, lambda i, tab: (0, 0, 0)),
                ANY,
                ANY,
                ANY,
                ANY,
            ],
            out_specs=block,
            scratch_shapes=[
                pltpu.VMEM((2, BLOCKS, 2, STRETCH, width), jnp.bfloat16),
                pltpu.SemaphoreType.DMA((2, BLOCKS)),
            ],
        ),
        compiler_params=pltpu.CompilerParams(
            dimension_semantics=("arbitrary",), vmem_limit_bytes=60 * 1024 * 1024
        ),
        name="attend",
    )(table, queries, pooled, own, before, after, routed)


def shot_sources(shot_bounds, position, stretch_count):
    first = shot_bounds[:, 0] - position * stretch_count
    live = shot_bounds[:, 1] - shot_bounds[:, 0]
    steps = jnp.arange(SHOT_MAX)[None, :]
    local = first[:, None] + jnp.where(steps < live[:, None], steps, 0)
    source = jnp.where(local < 0, 1, jnp.where(local >= stretch_count, 2, 0))
    index = jnp.where(local < 0, local + RIM, jnp.where(local >= stretch_count, local - stretch_count, local))
    return source, index, live


def body(queries, keys_values, shot_bounds, routes):
    width = keys_values.shape[2]
    stretch_count = queries.shape[0] // STRETCH
    device_count = lax.axis_size("seq")
    position = lax.axis_index("seq")
    request_count = stretch_count * TOPK
    capacity = max(2, (request_count + device_count - 1) // device_count)

    flattened = routes.reshape(-1)
    owners, held = flattened // stretch_count, flattened % stretch_count
    owner_hot = (owners[:, None] == jnp.arange(device_count)[None, :]).astype(jnp.int32)
    ranking = jnp.sum((jnp.cumsum(owner_hot, axis=0) - owner_hot) * owner_hot, axis=1)
    slots = owners * capacity + ranking
    slot_hot = (slots[:, None] == jnp.arange(device_count * capacity)[None, :]).astype(jnp.int32)
    slot_table = jnp.sum(slot_hot * held[:, None], axis=0).reshape(device_count, capacity)
    wanted = lax.all_to_all(slot_table, "seq", split_axis=0, concat_axis=0, tiled=True)

    before, after = edge_stretches(keys_values, RIM * STRETCH)
    kv_stretches = keys_values.reshape(2, stretch_count, STRETCH, width)
    pooled_local = jnp.mean(kv_stretches, axis=2, dtype=jnp.float32).astype(jnp.bfloat16)
    pooled = lax.all_gather(pooled_local, "seq", axis=1, tiled=True)

    outgoing = jnp.take(jnp.moveaxis(kv_stretches, 1, 0), wanted.reshape(-1), axis=0)
    arrived = lax.all_to_all(outgoing, "seq", split_axis=0, concat_axis=0, tiled=True)

    source, index, live = shot_sources(shot_bounds, position, stretch_count)
    slots = slots.reshape(stretch_count, TOPK)
    source = jnp.concatenate([source, jnp.full_like(slots, 3)], axis=1)
    index = jnp.concatenate([index, slots], axis=1)
    table = jnp.stack([source, index], axis=2).reshape(stretch_count, 2 * BLOCKS)
    table = jnp.concatenate([table, live[:, None]], axis=1).astype(jnp.int32)
    return attend(table, queries, pooled, keys_values, before, after, arrived)


def solution(mesh):
    in_specs = (
        P(("groups", "seq"), "head"),
        P(None, ("groups", "seq"), "head"),
        P(("groups", "seq"), None),
        P(("groups", "seq"), None),
    )
    out_specs = P(("groups", "seq"), "head")
    return jax.shard_map(body, mesh=mesh, in_specs=in_specs, out_specs=out_specs, check_vma=False)
```
